32 devices in a mesh: grp: 2 (over y), tp: 8 (over z, x), sub: 2 (over core).
Axes of the slice: x: 2, y: 2, z: 4, core: 2. Of those that a mesh axis runs over, the one named last changes fastest.
Arguments:
- hidden_in: bfloat16 [32, 2, 4096], P('grp', 'sub', 'tp'), parts along dimension 0, may hold values from -16 to 16
- norm_attn: float32 [8192], replicated, may hold values from 0.25 to 1.75
- w_query: bfloat16 [8192, 2, 4096], P(None, 'sub', 'tp'), may hold values from -0.0625 to 0.0625
- w_key: bfloat16 [8192, 2, 512], P(None, 'sub', 'tp'), may hold values from -0.0625 to 0.0625
- w_value: bfloat16 [8192, 2, 512], P(None, 'sub', 'tp'), may hold values from -0.0625 to 0.0625
- w_out: bfloat16 [2, 4096, 2, 4096], P('sub', None, None, 'tp'), may hold values from -0.0625 to 0.0625
- norm_ffn: float32 [8192], replicated, may hold values from 0.25 to 1.75
- w_gate: bfloat16 [2, 4096, 14336], P('sub', None, 'tp'), may hold values from -0.0625 to 0.0625
- w_up: bfloat16 [2, 4096, 14336], P('sub', None, 'tp'), may hold values from -0.0625 to 0.0625
- w_down: bfloat16 [14336, 2, 4096], P('tp', 'sub'), may hold values from -0.0625 to 0.0625
- cache_keys: bfloat16 [32, 64, 8, 128], P('grp', 'tp', 'sub'), parts along dimension 0, may hold values from -250 to 250
- cache_values: bfloat16 [32, 64, 8, 128], P('grp', 'tp', 'sub'), parts along dimension 0, may hold values from -6 to 6
- lengths: int32 [32], P('grp'), parts along dimension 0, may hold values from 1 to 64, as said below
Outputs:
- hidden_out: bfloat16 [32, 2, 4096], P('grp', 'sub', 'tp'), parts along dimension 0
The draws below stay inside these ranges and needn't reach their ends.
There are 2 independent parts, one for each index of `grp`. The reference program is written for one: setup_inputs(seed, part) draws one part's arguments, and reference() takes and returns one part's arrays. A program takes and returns all parts, laid end to end along the dimension named above; an argument that names none is the same for every part. Nothing has to cross between parts.
Inputs may be any that keep to these rules, and one draw needn't show every extreme that they name: `lengths`: some sequence has 64 live positions and some has 1.
All inputs are finite; a program needn't handle non-finite values.
Results may differ from the reference program's by a relative error of at most 0.012.
The reference program's roundings to bfloat16 on the way (of `normed`, `attended`, `middle`, `normed_ffn` and `hidden`) count: a program that leaves them out, or rounds other values in their place, can miss the bound.
Values may be sent and summed in bfloat16 or wider, within the bound.
A program may use at most 128 MiB of HBM per device.

```python
import math
import jax
import jax.numpy as jnp
from jax import lax

D = 8192
HQ = 64
HK = 8
HD = 128
FF = 14336
SEQS = 16
CACHE_LEN = 64
N_SUB = 2


def draw_hidden_in(key, part):
    base_key = jax.random.fold_in(key, 101)
    key_noise, key_rows, key_cols = jax.random.split(base_key, 3)
    ramp = jnp.sqrt(1.0 + 2.0 * jnp.arange(D, dtype=jnp.float32) / (D - 1))
    noise = jnp.clip(jax.random.normal(key_noise, (SEQS, D), jnp.float32), -4.0, 4.0)
    row_scale = jnp.exp(jax.random.uniform(key_rows, (SEQS, 1), jnp.float32, math.log(0.5), math.log(2.0)))
    column_scale = jnp.exp(jax.random.uniform(key_cols, (1, D), jnp.float32, math.log(0.5), math.log(2.0)))
    values = jnp.clip(noise * row_scale * column_scale * ramp[None, :], -16.0, 16.0)
    return values.reshape(SEQS, N_SUB, D // N_SUB).astype(jnp.bfloat16)


def draw_cache_keys(key, part):
    base_key = jax.random.fold_in(key, 202)
    key_noise, key_pick, key_strength = jax.random.split(base_key, 3)
    noise = jnp.clip(jax.random.normal(key_noise, (SEQS, CACHE_LEN, HK, HD), jnp.float32), -2.0, 2.0)
    strength = jnp.exp(jax.random.uniform(key_strength, (SEQS, CACHE_LEN), jnp.float32, math.log(40.0), math.log(120.0)))
    picked = jax.random.uniform(key_pick, (SEQS, CACHE_LEN), jnp.float32) < 0.1
    boosted = noise * jnp.where(picked, strength, 1.0)[:, :, None, None]
    twins = jnp.concatenate([boosted[:, :1], boosted[:, :-1] * 1.01], axis=1)
    follows = jnp.concatenate([jnp.zeros((SEQS, 1), dtype=bool), picked[:, :-1]], axis=1)
    values = jnp.where(follows[:, :, None, None], twins, boosted)
    return jnp.clip(values, -250.0, 250.0).astype(jnp.bfloat16)


def draw_lengths(key, part):
    base_key = jax.random.fold_in(key, 303)
    key_values, key_order = jax.random.split(base_key, 2)
    values = jax.random.randint(key_values, (SEQS,), 1, CACHE_LEN + 1, dtype=jnp.int32)
    order = jax.random.permutation(key_order, SEQS)
    values = values.at[order[0]].set(CACHE_LEN)
    values = values.at[order[1]].set(1)
    return values.astype(jnp.int32)


def raised(values, key, source, target, blocks, factor):
    owner, partner = [(jnp.arange(values.shape[position]) // (values.shape[position] // blocks)).reshape([-1 if axis == position else 1 for axis in range(values.ndim)]) for position in (source, target)]
    chosen = jax.random.permutation(key, blocks)[partner]
    strong = (owner == chosen) | (owner == (partner + blocks // 2) % blocks)
    return jnp.where(strong, factor * values, values)


def block_scale(own_key, dims, pieces, smallest, top_value):
    def one(dim, shards_of):
        heights = jax.random.uniform(jax.random.fold_in(jax.random.fold_in(own_key, 6), dim), (shards_of,), jnp.float32, smallest / len(pieces), top_value / len(pieces))
        return jnp.repeat(jnp.exp(heights), dims[dim] // shards_of).reshape((-1,) + (1,) * (len(dims) - dim - 1))

    factor_of = one(*pieces[0])
    for cut in pieces[1:]:
        factor_of = factor_of * one(*cut)
    return factor_of


def normal_values(rng, extent, spread, limit, cuts=(), kind=jnp.bfloat16):
    array = spread * jax.random.normal(rng, extent, jnp.float32)
    if cuts:
        array = array * block_scale(rng, extent, cuts, -0.22, 0.18)
    return jnp.clip(array, -limit, limit).astype(kind)


def bell_draw_with(key, dims, deviation, bound, pieces, heavy, held_as=jnp.bfloat16):
    array = deviation * jax.random.normal(key, dims, jnp.float32)
    if pieces:
        array = array * block_scale(key, dims, pieces, -0.22, 0.18)
    return jnp.clip(raised(array, jax.random.fold_in(key, 3), *heavy), -bound, bound).astype(held_as)


def setup_inputs(seed: int = 0, part: int = 0) -> dict:
    arg_keys = jax.random.split(jax.random.key(seed), 14)
    part_splits = jax.random.split(jax.random.fold_in(arg_keys[13], part), 14)
    hidden_in = draw_hidden_in(jax.random.fold_in(jax.random.fold_in(arg_keys[13], part), 71), part)
    norm_attn = jnp.clip(1.0 + 0.15 * jax.random.normal(arg_keys[1], (D,), jnp.float32), 0.25, 1.75)
    w_query = normal_values(arg_keys[2], (D, N_SUB, HQ * HD // N_SUB), D ** -0.5, 0.0625, ((1, 2), (2, 8)))
    w_key = normal_values(arg_keys[3], (D, N_SUB, HK * HD // N_SUB), D ** -0.5, 0.0625, ((1, 2), (2, 8)))
    w_value = normal_values(arg_keys[4], (D, N_SUB, HK * HD // N_SUB), D ** -0.5, 0.0625, ((1, 2), (2, 8)))
    w_out = normal_values(arg_keys[5], (N_SUB, HQ * HD // N_SUB, N_SUB, D // N_SUB), (HQ * HD) ** -0.5, 0.0625, ((0, 2), (3, 8)))
    norm_ffn = jnp.clip(1.0 + 0.15 * jax.random.normal(arg_keys[6], (D,), jnp.float32), 0.25, 1.75)
    w_gate = normal_values(arg_keys[7], (N_SUB, D // N_SUB, FF), D ** -0.5, 0.0625, ((0, 2), (2, 8)))
    w_up = normal_values(arg_keys[8], (N_SUB, D // N_SUB, FF), D ** -0.5, 0.0625, ((0, 2), (2, 8)))
    w_down = bell_draw_with(arg_keys[9], (FF, N_SUB, D // N_SUB), FF ** -0.5, 0.0625, ((0, 8), (1, 2)), (0, 2, 8, 2.0))
    cache_keys = draw_cache_keys(jax.random.fold_in(jax.random.fold_in(arg_keys[13], part), 71), part)
    cache_values = normal_values(part_splits[11], (SEQS, CACHE_LEN, HK, HD), 1.0, 6.0, ((1, 8), (2, 2)))
    lengths = draw_lengths(jax.random.fold_in(jax.random.fold_in(arg_keys[13], part), 71), part)
    return {"hidden_in": hidden_in, "norm_attn": norm_attn, "w_query": w_query, "w_key": w_key, "w_value": w_value, "w_out": w_out, "norm_ffn": norm_ffn, "w_gate": w_gate, "w_up": w_up, "w_down": w_down, "cache_keys": cache_keys, "cache_values": cache_values, "lengths": lengths}


epsilon = 1e-05
rope_base = 500000.0
floor_score = -1e+30

def rms_norm(values, gain):
    mean_square = lax.optimization_barrier(jnp.mean(values * values, axis=-1, keepdims=True))
    return (values * lax.rsqrt(mean_square + epsilon) * gain.astype(jnp.float32)).astype(jnp.bfloat16)

def rope_angles(lengths):
    frequencies = rope_base ** (-(jnp.arange(HD // 2, dtype=jnp.float32) * 2.0) / HD)
    return lengths.astype(jnp.float32)[:, None] * frequencies[None, :]

def rotate(vectors, angles):
    middle_index = vectors.shape[-1] // 2
    cosine = jnp.cos(angles)[:, None, :]
    sine = jnp.sin(angles)[:, None, :]
    lower = vectors[..., :middle_index]
    upper = vectors[..., middle_index:]
    return jnp.concatenate([lower * cosine - upper * sine, upper * cosine + lower * sine], axis=-1)

def reference(hidden_in, norm_attn, w_query, w_key, w_value, w_out, norm_ffn, w_gate, w_up, w_down, cache_keys, cache_values, lengths):
    residual = hidden_in.reshape(SEQS, D).astype(jnp.float32)
    normed = rms_norm(residual, norm_attn)
    query = jnp.dot(normed, w_query.reshape(D, HQ * HD), preferred_element_type=jnp.float32).astype(jnp.bfloat16)
    key_new = jnp.dot(normed, w_key.reshape(D, HK * HD), preferred_element_type=jnp.float32).astype(jnp.bfloat16)
    value_new = jnp.dot(normed, w_value.reshape(D, HK * HD), preferred_element_type=jnp.float32).astype(jnp.bfloat16)
    angles = rope_angles(lengths)
    query_rot = rotate(query.astype(jnp.float32).reshape(SEQS, HQ, HD), angles).astype(jnp.bfloat16)
    key_rot = rotate(key_new.astype(jnp.float32).reshape(SEQS, HK, HD), angles).astype(jnp.bfloat16)
    group_size = HQ // HK
    grouped = query_rot.astype(jnp.float32).reshape(SEQS, HK, group_size, HD)
    scores = jnp.einsum('bkgd,blkd->bkgl', grouped, cache_keys.astype(jnp.float32), precision=lax.Precision.HIGHEST) / math.sqrt(HD)
    places = jnp.arange(cache_keys.shape[1], dtype=jnp.int32)
    live = (places[None, :] < lengths[:, None])[:, None, None, :]
    masked = jnp.where(live, scores, floor_score)
    own_score = lax.optimization_barrier(jnp.sum(grouped * key_rot.astype(jnp.float32)[:, :, None, :], axis=-1)) / math.sqrt(HD)
    highest = jnp.maximum(lax.optimization_barrier(jnp.max(masked, axis=-1)), own_score)
    weights = jnp.where(live, jnp.exp(masked - highest[..., None]), 0.0)
    own_weight = jnp.exp(own_score - highest)
    numerator = jnp.einsum('bkgl,blkd->bkgd', weights, cache_values.astype(jnp.float32), precision=lax.Precision.HIGHEST)
    numerator = numerator + own_weight[..., None] * value_new.astype(jnp.float32).reshape(SEQS, HK, 1, HD)
    denominator = lax.optimization_barrier(jnp.sum(weights, axis=-1)) + own_weight
    attended = (numerator / denominator[..., None]).reshape(SEQS, HQ * HD).astype(jnp.bfloat16)
    mixed = jnp.dot(attended, w_out.reshape(HQ * HD, D), preferred_element_type=jnp.float32)
    middle = (residual + mixed).astype(jnp.bfloat16)
    normed_ffn = rms_norm(middle.astype(jnp.float32), norm_ffn)
    gate = jnp.dot(normed_ffn, w_gate.reshape(D, FF), preferred_element_type=jnp.float32)
    up_value = jnp.dot(normed_ffn, w_up.reshape(D, FF), preferred_element_type=jnp.float32)
    hidden = (jax.nn.silu(gate) * up_value).astype(jnp.bfloat16)
    down_value = jnp.dot(hidden, w_down.reshape(FF, D), preferred_element_type=jnp.float32)
    result = (middle.astype(jnp.float32) + down_value).astype(jnp.bfloat16)
    return result.reshape(SEQS, N_SUB, D // N_SUB)
```

```python
import functools
import math

import jax
import jax.numpy as jnp
from jax import lax
from jax.experimental import pallas as pl
from jax.experimental.pallas import tpu as pltpu
from jax.sharding import PartitionSpec as P

HD = 128


epsilon = 1e-05
rope_base = 500000.0
floor_score = -1e30


def joined(part, axis, combine):
    gathered = jax.tree.map(lambda a: lax.all_gather(a, axis), part)

    def take(source):
        return jax.tree.map(lambda a: lax.dynamic_index_in_dim(a, source, 0, False), gathered)

    return lax.fori_loop(
        1, lax.axis_size(axis), lambda source, state: combine(state, take(source)), take(0)
    )


def rope_angles(lengths):
    frequencies = rope_base ** (-(jnp.arange(HD // 2, dtype=jnp.float32) * 2.0) / HD)
    return lengths.astype(jnp.float32)[:, None] * frequencies[None, :]


def rotate(vectors, angles):
    middle_index = vectors.shape[-1] // 2
    cosine = jnp.cos(angles)[:, None, :]
    sine = jnp.sin(angles)[:, None, :]
    lower = vectors[..., :middle_index]
    upper = vectors[..., middle_index:]
    return jnp.concatenate([lower * cosine - upper * sine, upper * cosine + lower * sine], axis=-1)


def spread_rows(shard):
    across = lax.all_gather(shard, "tp", axis=2, tiled=True)
    return lax.all_gather(across, "sub", axis=1, tiled=True)


def half_rows_of(shard):
    return lax.all_gather(shard, "tp", axis=2, tiled=True)


def join_partials(earlier, later):
    earlier_max, earlier_sum, earlier_out = earlier
    later_max, later_sum, later_out = later
    highest = jnp.maximum(earlier_max, later_max)
    earlier_scale = jnp.exp(earlier_max - highest)
    later_scale = jnp.exp(later_max - highest)
    joined_sum = earlier_sum * earlier_scale + later_sum * later_scale
    joined_out = earlier_out * earlier_scale[..., None] + later_out * later_scale[..., None]
    return (highest, joined_sum, joined_out)


def per_device_plain(
    hidden_in,
    norm_attn,
    w_query,
    w_key,
    w_value,
    w_out,
    norm_ffn,
    w_gate,
    w_up,
    w_down,
    cache_keys,
    cache_values,
    lengths,
):
    seq_count = hidden_in.shape[0]
    shard_width = hidden_in.shape[2]
    half_width = shard_width * lax.axis_size("tp")
    model_width = half_width * lax.axis_size("sub")
    tp_pos = lax.axis_index("tp")
    sub_pos = lax.axis_index("sub")
    residual = hidden_in.astype(jnp.float32)
    whole_rows = spread_rows(hidden_in).astype(jnp.float32)
    factor = lax.rsqrt(jnp.mean(whole_rows * whole_rows, axis=(1, 2)) + epsilon)
    gain_whole = norm_attn.reshape(whole_rows.shape[1], half_width)
    gathered = (whole_rows * factor[:, None, None] * gain_whole).astype(jnp.bfloat16)
    flattened = gathered.reshape(seq_count, model_width)
    query_part = jnp.dot(
        flattened, w_query.reshape(model_width, -1), preferred_element_type=jnp.float32
    ).astype(jnp.bfloat16)
    key_part = jnp.dot(
        flattened, w_key.reshape(model_width, -1), preferred_element_type=jnp.float32
    ).astype(jnp.bfloat16)
    value_part = jnp.dot(
        flattened, w_value.reshape(model_width, -1), preferred_element_type=jnp.float32
    ).astype(jnp.bfloat16)
    query, key_new, value_new = (
        lax.all_gather(query_part, "tp", axis=1, tiled=True),
        lax.all_gather(key_part, "tp", axis=1, tiled=True),
        lax.all_gather(value_part, "tp", axis=1, tiled=True),
    )
    query_heads = query.shape[1] // HD
    kv_heads = key_new.shape[1] // HD
    group_size = query_heads // kv_heads
    angles = rope_angles(lengths)
    query_rot = rotate(
        query.astype(jnp.float32).reshape(seq_count, query_heads, HD), angles
    ).astype(jnp.bfloat16)
    key_rot = rotate(key_new.astype(jnp.float32).reshape(seq_count, kv_heads, HD), angles).astype(
        jnp.bfloat16
    )
    grouped = query_rot.reshape(seq_count, kv_heads, group_size, HD)
    values_new = value_new.astype(jnp.float32).reshape(seq_count, kv_heads, 1, HD)
    span = cache_keys.shape[1]
    scores = jnp.einsum(
        "bkgd,blkd->bkgl", grouped, cache_keys, preferred_element_type=jnp.float32
    ) / math.sqrt(HD)
    places = tp_pos * span + jnp.arange(span, dtype=jnp.int32)
    live = (places[None, :] < lengths[:, None])[:, None, None, :]
    masked = jnp.where(live, scores, floor_score)
    local_max = jnp.max(masked, axis=-1)
    weights = jnp.where(live, jnp.exp(masked - local_max[..., None]), 0.0)
    local_sum = jnp.sum(weights, axis=-1)
    local_out = jnp.einsum(
        "bkgl,blkd->bkgd",
        weights,
        cache_values.astype(jnp.float32),
        precision=lax.Precision.HIGHEST,
    )
    own_score = jnp.sum(
        grouped.astype(jnp.float32) * key_rot.astype(jnp.float32)[:, :, None, :], axis=-1
    ) / math.sqrt(HD)
    joined_max, joined_sum, joined_out = joined(
        (local_max, local_sum, local_out), "tp", join_partials
    )
    highest = jnp.maximum(joined_max, own_score)
    kept_scale = jnp.exp(joined_max - highest)
    own_weight = jnp.exp(own_score - highest)
    numerator = joined_out * kept_scale[..., None] + own_weight[..., None] * values_new
    denominator = joined_sum * kept_scale + own_weight
    attended = (numerator / denominator[..., None]).reshape(seq_count, -1).astype(jnp.bfloat16)
    out_part = jnp.dot(
        attended, w_out.reshape(attended.shape[1], -1), preferred_element_type=jnp.float32
    )
    out_part = out_part.reshape(seq_count, -1, shard_width)
    mixed = lax.psum_scatter(out_part, "sub", scatter_dimension=1, tiled=True)
    middle = (residual + mixed).astype(jnp.bfloat16)
    middle_float = middle.astype(jnp.float32)
    raw_half = half_rows_of(middle).astype(jnp.float32)
    partial_squares = jnp.sum(raw_half * raw_half, axis=(1, 2))
    squares_mid = lax.psum(partial_squares, "sub")
    factor_mid = lax.rsqrt(squares_mid / model_width + epsilon)
    gain_half = lax.dynamic_slice_in_dim(norm_ffn, sub_pos * half_width, half_width)
    half_rows = (raw_half * factor_mid[:, None, None] * gain_half).astype(jnp.bfloat16)
    half_flat = half_rows.reshape(seq_count, half_width)
    gate_part = jnp.dot(
        half_flat, w_gate.reshape(half_width, -1), preferred_element_type=jnp.float32
    )
    up_part = jnp.dot(half_flat, w_up.reshape(half_width, -1), preferred_element_type=jnp.float32)
    gate_total, up_total = lax.psum((gate_part, up_part), "sub")
    hidden = (jax.nn.silu(gate_total) * up_total).astype(jnp.bfloat16)
    down_part = jnp.dot(
        hidden, w_down.reshape(hidden.shape[1], -1), preferred_element_type=jnp.float32
    )
    down_total = lax.psum(down_part, "tp")
    down_share = lax.dynamic_slice_in_dim(down_total, tp_pos * shard_width, shard_width, 1)
    return (middle_float + down_share[:, None, :]).astype(jnp.bfloat16)


MESH_ID = pl.DeviceIdType.MESH
F32 = jnp.float32
BF16 = jnp.bfloat16
NT = (((1,), (1,)), ((), ()))


def matmul(a, b):
    return jnp.dot(a, b, preferred_element_type=F32)


def remote(src, dst, send, recv, tp, sub):
    return pltpu.make_async_remote_copy(
        src_ref=src,
        dst_ref=dst,
        send_sem=send,
        recv_sem=recv,
        device_id={"tp": tp, "sub": sub},
        device_id_type=MESH_ID,
    )


def step_kernel(
    cfg,
    x_ref,
    aux_ref,
    gain1_ref,
    gain2_ref,
    wq_hbm,
    wk_hbm,
    wv_hbm,
    wo_hbm,
    wg_hbm,
    wu_hbm,
    wd_hbm,
    ck_hbm,
    cv_hbm,
    out_ref,
    wq,
    wk,
    wv,
    wo,
    wg,
    wu,
    wd,
    xg,
    ckr,
    cvr,
    qkv,
    qs,
    qr,
    ascr,
    arow,
    ab,
    attf,
    attb,
    op,
    orv,
    mg,
    nf,
    gp,
    gr,
    hid,
    dp,
    dr,
    w_sem,
    c_sem,
    xs_sem,
    xr_sem,
    cks_sem,
    ckr_sem,
    cvs_sem,
    cvr_sem,
    qs_sem,
    qr_sem,
    as_sem,
    ar_sem,
    o_sem,
    ms_sem,
    mr_sem,
    gs_sem,
    gr_sem,
    ds_sem,
    dr_sem,
):
    tp_n, sub_n, own, hpd, span, kvh = cfg
    peers = tp_n * sub_n
    seqs, width = x_ref.shape
    model = peers * width
    half = tp_n * width
    t = lax.axis_index("tp")
    s = lax.axis_index("sub")
    me = s * tp_n + t

    def load(i, src, dst):
        return pltpu.make_async_copy(src, dst, w_sem.at[i])

    loads = [
        load(i, a, b)
        for i, (a, b) in enumerate(
            (
                (wq_hbm, wq),
                (wk_hbm, wk),
                (wv_hbm, wv),
                (wo_hbm, wo),
                (wg_hbm, wg),
                (wu_hbm, wu),
                (wd_hbm, wd),
            )
        )
    ]
    for c in loads[:3]:
        c.start()

    barrier = pltpu.get_barrier_semaphore()

    def greet(k, carry):
        peer = lax.rem(me + k, peers)
        pl.semaphore_signal(
            barrier,
            inc=1,
            device_id={"tp": lax.rem(peer, tp_n), "sub": peer // tp_n},
            device_id_type=MESH_ID,
        )
        return carry

    lax.fori_loop(1, peers, greet, 0)
    pl.semaphore_wait(barrier, peers - 1)

    def spread(src, buf, ssem, rsem):
        def one(k, carry):
            peer = lax.rem(me + k, peers)
            remote(
                src, buf.at[me], ssem.at[k], rsem.at[me], lax.rem(peer, tp_n), peer // tp_n
            ).start()
            return carry

        lax.fori_loop(1, peers, one, 0)

    def spread_wait(buf, ssem, rsem):
        def one(k, carry):
            peer = lax.rem(me + k, peers)
            remote(buf.at[peer], buf.at[peer], ssem.at[k], rsem.at[peer], t, s).wait_recv()
            return carry

        lax.fori_loop(1, peers, one, 0)

    def spread_done(src, ssem, rsem):
        def one(k, carry):
            remote(src, src, ssem.at[k], rsem.at[me], t, s).wait_send()
            return carry

        lax.fori_loop(1, peers, one, 0)

    def send_tp(src_of, buf, ssem, rsem):
        def one(k, carry):
            peer = lax.rem(t + k, tp_n)
            remote(src_of(peer), buf.at[t], ssem.at[k], rsem.at[t], peer, s).start()
            return carry

        lax.fori_loop(1, tp_n, one, 0)

    def wait_tp(buf, ssem, rsem):
        def one(k, carry):
            peer = lax.rem(t + k, tp_n)
            remote(buf.at[peer], buf.at[peer], ssem.at[k], rsem.at[peer], t, s).wait_recv()
            return carry

        lax.fori_loop(1, tp_n, one, 0)

    def done_tp(src_of, buf, ssem, rsem):
        def one(k, carry):
            peer = lax.rem(t + k, tp_n)
            remote(src_of(peer), buf.at[t], ssem.at[k], rsem.at[t], peer, s).wait_send()
            return carry

        lax.fori_loop(1, tp_n, one, 0)

    spread(x_ref, xg, xs_sem, xr_sem)
    xg[me] = x_ref[...]

    def ck_of(peer):
        return ck_hbm.at[pl.ds(peer * own, own)]

    def cv_of(peer):
        return cv_hbm.at[pl.ds(peer * own, own)]

    send_tp(ck_of, ckr, cks_sem, ckr_sem)
    send_tp(cv_of, cvr, cvs_sem, cvr_sem)
    own_k = pltpu.make_async_copy(ck_of(t), ckr.at[t], c_sem.at[0])
    own_v = pltpu.make_async_copy(cv_of(t), cvr.at[t], c_sem.at[1])
    own_k.start()
    own_v.start()
    loads[3].start()

    spread_wait(xg, xs_sem, xr_sem)

    def squares(c, acc):
        v = xg[c].astype(F32)
        return acc + jnp.sum(v * v, axis=1, keepdims=True)

    total = lax.fori_loop(0, peers, squares, jnp.zeros((seqs, 1), F32))
    factor = lax.rsqrt(total / model + epsilon)
    for c in loads[:3]:
        c.wait()
    for c in loads[4:]:
        c.start()

    def project(c, carry):
        q, k, v = carry
        at = pl.ds(pl.multiple_of(c * width, width), width)
        n = (xg[c].astype(F32) * factor * gain1_ref[:, at]).astype(BF16)
        q = q + matmul(n, wq[at, :])
        k = k + lax.dot_general(n, wk[:, at], NT, preferred_element_type=F32)
        v = v + lax.dot_general(n, wv[:, at], NT, preferred_element_type=F32)
        return q, k, v

    kvw = wk.shape[0]
    q, k, v = lax.fori_loop(
        0,
        peers,
        project,
        (
            jnp.zeros((seqs, width), F32),
            jnp.zeros((seqs, kvw), F32),
            jnp.zeros((seqs, kvw), F32),
        ),
    )
    parts = HD // kvw
    lane = lax.broadcasted_iota(jnp.int32, (seqs, HD), 1)
    mine = lane // kvw == lax.rem(t, parts)
    qkv[:, :width] = q.astype(BF16).astype(F32)
    for n, value in enumerate((k, v)):
        whole = jnp.concatenate([value.astype(BF16).astype(F32)] * parts, axis=1)
        qkv[:, width + n * HD : width + (n + 1) * HD] = jnp.where(mine, whole, 0.0)
    for d in range(tp_n):
        qs[d] = qkv[d * own : (d + 1) * own, :]
    qr[t] = qs[t]
    send_tp(lambda peer: qs.at[peer], qr, qs_sem, qr_sem)

    wait_tp(ckr, cks_sem, ckr_sem)
    wait_tp(cvr, cvs_sem, cvr_sem)
    own_k.wait()
    own_v.wait()
    wait_tp(qr, qs_sem, qr_sem)

    rows = hpd * tp_n
    cols = tp_n * span * kvh
    row = lax.broadcasted_iota(jnp.int32, (rows, cols), 0)
    col = lax.broadcasted_iota(jnp.int32, (rows, cols), 1)
    same_head = lax.rem(row, tp_n) // parts == lax.rem(col, kvh)
    place = (col // kvh).astype(F32)
    pair_row = lax.broadcasted_iota(jnp.int32, (tp_n, tp_n), 0)
    pair_col = lax.broadcasted_iota(jnp.int32, (tp_n, tp_n), 1)
    pairs = jnp.where(pair_row // parts == pair_col // parts, 1.0, 0.0).astype(F32)
    root = math.sqrt(HD)

    def rope(value, cosine, sine):
        turned = pltpu.roll(value, HD // 2, 1)
        return (value * cosine + turned * sine).astype(BF16)

    for i in range(own):
        table = aux_ref[t * own + i]
        cosine, sine, length = table[0:1], table[1:2], table[2:3, 0:1]
        queries = jnp.concatenate(
            [qr[:, i, j * HD : (j + 1) * HD] for j in range(hpd)], axis=0
        )
        query_rot = rope(queries, cosine, sine)
        exact = lax.Precision.HIGHEST
        key_new = jnp.dot(
            pairs, qr[:, i, width : width + HD], precision=exact, preferred_element_type=F32
        )
        value_new = jnp.dot(
            pairs,
            qr[:, i, width + HD : width + 2 * HD],
            precision=exact,
            preferred_element_type=F32,
        )
        key_rot = rope(key_new, cosine, sine).astype(F32)
        keys = ckr[:, i].reshape(cols, HD)
        values = cvr[:, i].reshape(cols, HD).astype(F32)
        scores = lax.dot_general(query_rot, keys, NT, preferred_element_type=F32) / root
        live = same_head & (place < length)
        masked = jnp.where(live, scores, floor_score)
        key_all = jnp.concatenate([key_rot] * hpd, axis=0)
        value_all = jnp.concatenate([value_new] * hpd, axis=0)
        own_score = jnp.sum(query_rot.astype(F32) * key_all, axis=1, keepdims=True) / root
        highest = jnp.maximum(jnp.max(masked, axis=1, keepdims=True), own_score)
        weights = jnp.where(live, jnp.exp(masked - highest), 0.0)
        own_weight = jnp.exp(own_score - highest)
        numerator = jnp.dot(weights, values, precision=exact, preferred_element_type=F32)
        numerator = numerator + own_weight * value_all
        denominator = jnp.sum(weights, axis=1, keepdims=True) + own_weight
        ascr[...] = numerator / denominator
        for j in range(hpd):
            for d in range(tp_n):
                r = j * tp_n + d
                head = d * hpd + j
                arow[i : i + 1, head * HD : (head + 1) * HD] = ascr[r : r + 1, :]
    ab[t] = arow[...].astype(BF16)
    send_tp(lambda peer: ab.at[t], ab, as_sem, ar_sem)
    wait_tp(ab, as_sem, ar_sem)
    for d in range(tp_n):
        attf[d * own : (d + 1) * own, :] = ab[d].astype(F32)
    attb[...] = attf[...].astype(BF16)

    loads[3].wait()

    def mix(c, acc):
        at = pl.ds(pl.multiple_of(c * width, width), width)
        return acc + matmul(attb[:, at], wo[at, :])

    mixed = lax.fori_loop(0, tp_n, mix, jnp.zeros((seqs, sub_n * width), F32))
    for c in range(sub_n):
        op[c] = mixed[:, c * width : (c + 1) * width]
    other = 1 - s
    swap = remote(op.at[other], orv, o_sem.at[0], o_sem.at[1], t, other)
    swap.start()
    swap.wait_recv()
    middle = (x_ref[...].astype(F32) + (op[s] + orv[...])).astype(BF16)
    mg[me] = middle
    spread(mg.at[me], mg, ms_sem, mr_sem)
    spread_wait(mg, ms_sem, mr_sem)

    def squares_mid(c, acc):
        v = mg[c].astype(F32)
        return acc + jnp.sum(v * v, axis=1, keepdims=True)

    total_mid = lax.fori_loop(0, peers, squares_mid, jnp.zeros((seqs, 1), F32))
    factor_mid = lax.rsqrt(total_mid / model + epsilon)

    def scale(c, carry):
        at = pl.ds(pl.multiple_of(c * width, width), width)
        gain_at = pl.ds(pl.multiple_of(s * half + c * width, width), width)
        raw = mg[s * tp_n + c].astype(F32)
        nf[:, at] = (raw * factor_mid * gain2_ref[:, gain_at]).astype(BF16)
        return carry

    lax.fori_loop(0, tp_n, scale, 0)
    loads[4].wait()
    loads[5].wait()
    chunks, _, _, chunk = gp.shape

    def gate_copy(n):
        return remote(gp.at[n], gr.at[n], gs_sem.at[n], gr_sem.at[n], t, other)

    def gates(n, carry):
        at = pl.ds(pl.multiple_of(n * chunk, chunk), chunk)
        normed = nf[...]
        gp[n, 0] = matmul(normed, wg[:, at])
        gp[n, 1] = matmul(normed, wu[:, at])
        gate_copy(n).start()
        return carry

    lax.fori_loop(0, chunks, gates, 0)

    def joins(n, carry):
        gate_copy(n).wait_recv()
        at = pl.ds(pl.multiple_of(n * chunk, chunk), chunk)
        gate = gp[n, 0] + gr[n, 0]
        up = gp[n, 1] + gr[n, 1]
        hid[:, at] = (gate / (1.0 + jnp.exp(-gate)) * up).astype(BF16)
        return carry

    lax.fori_loop(0, chunks, joins, 0)
    loads[6].wait()

    def down(peer):
        at = pl.ds(pl.multiple_of(peer * width, width), width)
        return matmul(hid[...], wd[:, at])

    def share(k, carry):
        peer = lax.rem(t + k, tp_n)
        dp[peer] = down(peer)
        remote(dp.at[peer], dr.at[t], ds_sem.at[k], dr_sem.at[t], peer, s).start()
        return carry

    lax.fori_loop(1, tp_n, share, 0)
    result = down(t)

    def gather(k, acc):
        peer = lax.rem(t + k, tp_n)
        remote(dr.at[peer], dr.at[peer], ds_sem.at[k], dr_sem.at[peer], t, s).wait_recv()
        return acc + dr[peer]

    result = lax.fori_loop(1, tp_n, gather, result)
    out_ref[...] = (mg[me].astype(F32) + result).astype(BF16)

    spread_done(x_ref, xs_sem, xr_sem)
    done_tp(ck_of, ckr, cks_sem, ckr_sem)
    done_tp(cv_of, cvr, cvs_sem, cvr_sem)
    done_tp(lambda peer: qs.at[peer], qr, qs_sem, qr_sem)
    done_tp(lambda peer: ab.at[t], ab, as_sem, ar_sem)
    swap.wait_send()
    spread_done(mg.at[me], ms_sem, mr_sem)

    def gates_done(n, carry):
        gate_copy(n).wait_send()
        return carry

    lax.fori_loop(0, chunks, gates_done, 0)
    done_tp(lambda peer: dp.at[peer], dr, ds_sem, dr_sem)


def per_device(
    hidden_in,
    norm_attn,
    w_query,
    w_key,
    w_value,
    w_out,
    norm_ffn,
    w_gate,
    w_up,
    w_down,
    cache_keys,
    cache_values,
    lengths,
):
    tp_n = lax.axis_size("tp")
    sub_n = lax.axis_size("sub")
    seqs, _, width = hidden_in.shape
    model = norm_attn.shape[0]
    half = width * tp_n
    kvw = w_key.shape[2]
    span, kvh = cache_keys.shape[1:3]
    ff = w_gate.shape[2]
    hpd = max(width // HD, 1)
    own = max(seqs // tp_n, 1)
    fits = (
        sub_n == 2
        and width % HD == 0
        and ff % HD == 0
        and seqs % tp_n == 0
        and HD % kvw == 0
        and w_query.shape[2] == width
        and hpd * (HD // kvw) * kvh == hpd * tp_n
        and (span * kvh) % 16 == 0
    )
    if not fits:
        return per_device_plain(
            hidden_in,
            norm_attn,
            w_query,
            w_key,
            w_value,
            w_out,
            norm_ffn,
            w_gate,
            w_up,
            w_down,
            cache_keys,
            cache_values,
            lengths,
        )
    peers = tp_n * sub_n
    angles = rope_angles(lengths)
    cosine = jnp.cos(angles)
    sine = jnp.sin(angles)
    long = jnp.broadcast_to(lengths.astype(F32)[:, None], (seqs, HD))
    aux = jnp.stack(
        [
            jnp.concatenate([cosine, cosine], axis=1),
            jnp.concatenate([-sine, sine], axis=1),
            long,
        ],
        axis=1,
    )
    aux = jnp.pad(aux, ((0, 0), (0, 5), (0, 0)))
    chunk = 2 * HD if ff % (2 * HD) == 0 else HD
    chunks = ff // chunk
    dma = pltpu.SemaphoreType.DMA
    vmem = pltpu.VMEM
    weights = [
        w_query.reshape(model, width),
        w_key.reshape(model, kvw).T,
        w_value.reshape(model, kvw).T,
        w_out.reshape(half, sub_n * width),
        w_gate.reshape(half, ff),
        w_up.reshape(half, ff),
        w_down.reshape(ff, half),
    ]
    caches = [
        cache_keys.reshape(seqs, span * kvh, HD),
        cache_values.reshape(seqs, span * kvh, HD),
    ]
    wide = width + 2 * HD
    out = pl.pallas_call(
        functools.partial(step_kernel, (tp_n, sub_n, own, hpd, span, kvh)),
        out_shape=jax.ShapeDtypeStruct((seqs, width), BF16),
        in_specs=[pl.BlockSpec(memory_space=pltpu.VMEM)] * 4
        + [pl.BlockSpec(memory_space=pl.ANY)] * 9,
        out_specs=pl.BlockSpec(memory_space=pltpu.VMEM),
        scratch_shapes=[vmem(w.shape, BF16) for w in weights]
        + [
            vmem((peers, seqs, width), BF16),
            vmem((tp_n, own, span * kvh, HD), BF16),
            vmem((tp_n, own, span * kvh, HD), BF16),
            vmem((seqs, wide), F32),
            vmem((tp_n, own, wide), F32),
            vmem((tp_n, own, wide), F32),
            vmem((hpd * tp_n, HD), F32),
            vmem((own, half), F32),
            vmem((tp_n, own, half), BF16),
            vmem((seqs, half), F32),
            vmem((seqs, half), BF16),
            vmem((sub_n, seqs, width), F32),
            vmem((seqs, width), F32),
            vmem((peers, seqs, width), BF16),
            vmem((seqs, half), BF16),
            vmem((chunks, 2, seqs, chunk), F32),
            vmem((chunks, 2, seqs, chunk), F32),
            vmem((seqs, ff), BF16),
            vmem((tp_n, seqs, width), F32),
            vmem((tp_n, seqs, width), F32),
            dma((7,)),
            dma((2,)),
            dma((peers,)),
            dma((peers,)),
            dma((tp_n,)),
            dma((tp_n,)),
            dma((tp_n,)),
            dma((tp_n,)),
            dma((tp_n,)),
            dma((tp_n,)),
            dma((tp_n,)),
            dma((tp_n,)),
            dma((2,)),
            dma((peers,)),
            dma((peers,)),
            dma((chunks,)),
            dma((chunks,)),
            dma((tp_n,)),
            dma((tp_n,)),
        ],
        compiler_params=pltpu.CompilerParams(
            collective_id=0, has_side_effects=True, vmem_limit_bytes=67043328
        ),
        name="decode_step",
    )(
        hidden_in.reshape(seqs, width),
        aux,
        norm_attn.reshape(1, model),
        norm_ffn.reshape(1, model),
        *weights,
        *caches,
    )
    return out.reshape(seqs, 1, width)


def solution(mesh):
    in_specs = (
        P("grp", "sub", "tp"),
        P(),
        P(None, "sub", "tp"),
        P(None, "sub", "tp"),
        P(None, "sub", "tp"),
        P("sub", None, None, "tp"),
        P(),
        P("sub", None, "tp"),
        P("sub", None, "tp"),
        P("tp", "sub", None),
        P("grp", "tp", "sub", None),
        P("grp", "tp", "sub", None),
        P("grp"),
    )
    out_specs = P("grp", "sub", "tp")
    return jax.shard_map(
        per_device, mesh=mesh, in_specs=in_specs, out_specs=out_specs, check_vma=False
    )
```

```python
import functools
import math

import jax
import jax.numpy as jnp
from jax import lax
from jax.experimental import pallas as pl
from jax.experimental.pallas import tpu as pltpu
from jax.sharding import PartitionSpec as P

HD = 128


epsilon = 1e-05
rope_base = 500000.0
floor_score = -1e30


def joined(part, axis, combine):
    gathered = jax.tree.map(lambda a: lax.all_gather(a, axis), part)

    def take(source):
        return jax.tree.map(lambda a: lax.dynamic_index_in_dim(a, source, 0, False), gathered)

    return lax.fori_loop(
        1, lax.axis_size(axis), lambda source, state: combine(state, take(source)), take(0)
    )


def rope_angles(lengths):
    frequencies = rope_base ** (-(jnp.arange(HD // 2, dtype=jnp.float32) * 2.0) / HD)
    return lengths.astype(jnp.float32)[:, None] * frequencies[None, :]


def rotate(vectors, angles):
    middle_index = vectors.shape[-1] // 2
    cosine = jnp.cos(angles)[:, None, :]
    sine = jnp.sin(angles)[:, None, :]
    lower = vectors[..., :middle_index]
    upper = vectors[..., middle_index:]
    return jnp.concatenate([lower * cosine - upper * sine, upper * cosine + lower * sine], axis=-1)


def spread_rows(shard):
    across = lax.all_gather(shard, "tp", axis=2, tiled=True)
    return lax.all_gather(across, "sub", axis=1, tiled=True)


def half_rows_of(shard):
    return lax.all_gather(shard, "tp", axis=2, tiled=True)


def join_partials(earlier, later):
    earlier_max, earlier_sum, earlier_out = earlier
    later_max, later_sum, later_out = later
    highest = jnp.maximum(earlier_max, later_max)
    earlier_scale = jnp.exp(earlier_max - highest)
    later_scale = jnp.exp(later_max - highest)
    joined_sum = earlier_sum * earlier_scale + later_sum * later_scale
    joined_out = earlier_out * earlier_scale[..., None] + later_out * later_scale[..., None]
    return (highest, joined_sum, joined_out)


def per_device_plain(
    hidden_in,
    norm_attn,
    w_query,
    w_key,
    w_value,
    w_out,
    norm_ffn,
    w_gate,
    w_up,
    w_down,
    cache_keys,
    cache_values,
    lengths,
):
    seq_count = hidden_in.shape[0]
    shard_width = hidden_in.shape[2]
    half_width = shard_width * lax.axis_size("tp")
    model_width = half_width * lax.axis_size("sub")
    tp_pos = lax.axis_index("tp")
    sub_pos = lax.axis_index("sub")
    residual = hidden_in.astype(jnp.float32)
    whole_rows = spread_rows(hidden_in).astype(jnp.float32)
    factor = lax.rsqrt(jnp.mean(whole_rows * whole_rows, axis=(1, 2)) + epsilon)
    gain_whole = norm_attn.reshape(whole_rows.shape[1], half_width)
    gathered = (whole_rows * factor[:, None, None] * gain_whole).astype(jnp.bfloat16)
    flattened = gathered.reshape(seq_count, model_width)
    query_part = jnp.dot(
        flattened, w_query.reshape(model_width, -1), preferred_element_type=jnp.float32
    ).astype(jnp.bfloat16)
    key_part = jnp.dot(
        flattened, w_key.reshape(model_width, -1), preferred_element_type=jnp.float32
    ).astype(jnp.bfloat16)
    value_part = jnp.dot(
        flattened, w_value.reshape(model_width, -1), preferred_element_type=jnp.float32
    ).astype(jnp.bfloat16)
    query, key_new, value_new = (
        lax.all_gather(query_part, "tp", axis=1, tiled=True),
        lax.all_gather(key_part, "tp", axis=1, tiled=True),
        lax.all_gather(value_part, "tp", axis=1, tiled=True),
    )
    query_heads = query.shape[1] // HD
    kv_heads = key_new.shape[1] // HD
    group_size = query_heads // kv_heads
    angles = rope_angles(lengths)
    query_rot = rotate(
        query.astype(jnp.float32).reshape(seq_count, query_heads, HD), angles
    ).astype(jnp.bfloat16)
    key_rot = rotate(key_new.astype(jnp.float32).reshape(seq_count, kv_heads, HD), angles).astype(
        jnp.bfloat16
    )
    grouped = query_rot.reshape(seq_count, kv_heads, group_size, HD)
    values_new = value_new.astype(jnp.float32).reshape(seq_count, kv_heads, 1, HD)
    span = cache_keys.shape[1]
    scores = jnp.einsum(
        "bkgd,blkd->bkgl", grouped, cache_keys, preferred_element_type=jnp.float32
    ) / math.sqrt(HD)
    places = tp_pos * span + jnp.arange(span, dtype=jnp.int32)
    live = (places[None, :] < lengths[:, None])[:, None, None, :]
    masked = jnp.where(live, scores, floor_score)
    local_max = jnp.max(masked, axis=-1)
    weights = jnp.where(live, jnp.exp(masked - local_max[..., None]), 0.0)
    local_sum = jnp.sum(weights, axis=-1)
    local_out = jnp.einsum(
        "bkgl,blkd->bkgd",
        weights,
        cache_values.astype(jnp.float32),
        precision=lax.Precision.HIGHEST,
    )
    own_score = jnp.sum(
        grouped.astype(jnp.float32) * key_rot.astype(jnp.float32)[:, :, None, :], axis=-1
    ) / math.sqrt(HD)
    joined_max, joined_sum, joined_out = joined(
        (local_max, local_sum, local_out), "tp", join_partials
    )
    highest = jnp.maximum(joined_max, own_score)
    kept_scale = jnp.exp(joined_max - highest)
    own_weight = jnp.exp(own_score - highest)
    numerator = joined_out * kept_scale[..., None] + own_weight[..., None] * values_new
    denominator = joined_sum * kept_scale + own_weight
    attended = (numerator / denominator[..., None]).reshape(seq_count, -1).astype(jnp.bfloat16)
    out_part = jnp.dot(
        attended, w_out.reshape(attended.shape[1], -1), preferred_element_type=jnp.float32
    )
    out_part = out_part.reshape(seq_count, -1, shard_width)
    mixed = lax.psum_scatter(out_part, "sub", scatter_dimension=1, tiled=True)
    middle = (residual + mixed).astype(jnp.bfloat16)
    middle_float = middle.astype(jnp.float32)
    raw_half = half_rows_of(middle).astype(jnp.float32)
    partial_squares = jnp.sum(raw_half * raw_half, axis=(1, 2))
    squares_mid = lax.psum(partial_squares, "sub")
    factor_mid = lax.rsqrt(squares_mid / model_width + epsilon)
    gain_half = lax.dynamic_slice_in_dim(norm_ffn, sub_pos * half_width, half_width)
    half_rows = (raw_half * factor_mid[:, None, None] * gain_half).astype(jnp.bfloat16)
    half_flat = half_rows.reshape(seq_count, half_width)
    gate_part = jnp.dot(
        half_flat, w_gate.reshape(half_width, -1), preferred_element_type=jnp.float32
    )
    up_part = jnp.dot(half_flat, w_up.reshape(half_width, -1), preferred_element_type=jnp.float32)
    gate_total, up_total = lax.psum((gate_part, up_part), "sub")
    hidden = (jax.nn.silu(gate_total) * up_total).astype(jnp.bfloat16)
    down_part = jnp.dot(
        hidden, w_down.reshape(hidden.shape[1], -1), preferred_element_type=jnp.float32
    )
    down_total = lax.psum(down_part, "tp")
    down_share = lax.dynamic_slice_in_dim(down_total, tp_pos * shard_width, shard_width, 1)
    return (middle_float + down_share[:, None, :]).astype(jnp.bfloat16)


MESH_ID = pl.DeviceIdType.MESH
F32 = jnp.float32
BF16 = jnp.bfloat16
NT = (((1,), (1,)), ((), ()))


def matmul(a, b):
    return jnp.dot(a, b, preferred_element_type=F32)


def remote(src, dst, send, recv, tp, sub):
    return pltpu.make_async_remote_copy(
        src_ref=src,
        dst_ref=dst,
        send_sem=send,
        recv_sem=recv,
        device_id={"tp": tp, "sub": sub},
        device_id_type=MESH_ID,
    )


def step_kernel(
    cfg,
    x_ref,
    aux_ref,
    gain1_ref,
    gain2_ref,
    wq_hbm,
    wk_hbm,
    wv_hbm,
    wo_hbm,
    wg_hbm,
    wu_hbm,
    wd_hbm,
    ck_hbm,
    cv_hbm,
    out_ref,
    wq,
    wk,
    wv,
    wo,
    wg,
    wu,
    wd,
    xg,
    ckr,
    cvr,
    qkv,
    qs,
    qr,
    ascr,
    arow,
    ab,
    attf,
    attb,
    op,
    orv,
    mg,
    nf,
    gp,
    gr,
    hid,
    dp,
    dr,
    w_sem,
    c_sem,
    xs_sem,
    xr_sem,
    cks_sem,
    ckr_sem,
    cvs_sem,
    cvr_sem,
    qs_sem,
    qr_sem,
    as_sem,
    ar_sem,
    o_sem,
    ms_sem,
    mr_sem,
    gs_sem,
    gr_sem,
    ds_sem,
    dr_sem,
    xf_sem,
    xh_sem,
    mf_sem,
    mh_sem,
):
    tp_n, sub_n, own, hpd, span, kvh = cfg
    peers = tp_n * sub_n
    seqs, width = x_ref.shape
    model = peers * width
    half = tp_n * width
    t = lax.axis_index("tp")
    s = lax.axis_index("sub")
    me = s * tp_n + t

    def load(i, src, dst):
        return pltpu.make_async_copy(src, dst, w_sem.at[i])

    loads = [
        load(i, a, b)
        for i, (a, b) in enumerate(
            (
                (wq_hbm, wq),
                (wk_hbm, wk),
                (wv_hbm, wv),
                (wo_hbm, wo),
                (wg_hbm, wg),
                (wu_hbm, wu),
                (wd_hbm, wd),
            )
        )
    ]
    for c in loads[:3]:
        c.start()

    barrier = pltpu.get_barrier_semaphore()

    def greet(k, carry):
        peer = lax.rem(me + k, peers)
        pl.semaphore_signal(
            barrier,
            inc=1,
            device_id={"tp": lax.rem(peer, tp_n), "sub": peer // tp_n},
            device_id_type=MESH_ID,
        )
        return carry

    lax.fori_loop(1, peers, greet, 0)
    pl.semaphore_wait(barrier, peers - 1)

    other = 1 - s

    def forward(src, buf, slot, peer, fsem, gsem):
        return remote(src, buf.at[slot], fsem.at[peer], gsem.at[peer], t, other)

    def spread(src, buf, ssem, rsem, fsem, gsem):
        forward(src, buf, me, t, fsem, gsem).start()

        def one(k, carry):
            peer = lax.rem(t + k, tp_n)
            remote(src, buf.at[me], ssem.at[k], rsem.at[t], peer, s).start()
            return carry

        lax.fori_loop(1, tp_n, one, 0)

    def spread_wait(buf, ssem, rsem, fsem, gsem):
        def one(k, carry):
            peer = lax.rem(t + k, tp_n)
            slot = s * tp_n + peer
            remote(buf.at[slot], buf.at[slot], ssem.at[k], rsem.at[peer], t, s).wait_recv()
            forward(buf.at[slot], buf, slot, peer, fsem, gsem).start()
            return carry

        lax.fori_loop(1, tp_n, one, 0)

        def two(peer, carry):
            slot = other * tp_n + peer
            forward(buf.at[slot], buf, slot, peer, fsem, gsem).wait_recv()
            return carry

        lax.fori_loop(0, tp_n, two, 0)

    def spread_done(src, buf, ssem, rsem, fsem, gsem):
        def one(k, carry):
            peer = lax.rem(t + k, tp_n)
            slot = s * tp_n + peer
            remote(src, buf.at[me], ssem.at[k], rsem.at[t], peer, s).wait_send()
            forward(buf.at[slot], buf, slot, peer, fsem, gsem).wait_send()
            return carry

        lax.fori_loop(1, tp_n, one, 0)
        forward(src, buf, me, t, fsem, gsem).wait_send()

    def send_tp(src_of, buf, ssem, rsem):
        def one(k, carry):
            peer = lax.rem(t + k, tp_n)
            remote(src_of(peer), buf.at[t], ssem.at[k], rsem.at[t], peer, s).start()
            return carry

        lax.fori_loop(1, tp_n, one, 0)

    def wait_tp(buf, ssem, rsem):
        def one(k, carry):
            peer = lax.rem(t + k, tp_n)
            remote(buf.at[peer], buf.at[peer], ssem.at[k], rsem.at[peer], t, s).wait_recv()
            return carry

        lax.fori_loop(1, tp_n, one, 0)

    def done_tp(src_of, buf, ssem, rsem):
        def one(k, carry):
            peer = lax.rem(t + k, tp_n)
            remote(src_of(peer), buf.at[t], ssem.at[k], rsem.at[t], peer, s).wait_send()
            return carry

        lax.fori_loop(1, tp_n, one, 0)

    spread(x_ref, xg, xs_sem, xr_sem, xf_sem, xh_sem)
    xg[me] = x_ref[...]

    def ck_of(peer):
        return ck_hbm.at[pl.ds(peer * own, own)]

    def cv_of(peer):
        return cv_hbm.at[pl.ds(peer * own, own)]

    send_tp(ck_of, ckr, cks_sem, ckr_sem)
    send_tp(cv_of, cvr, cvs_sem, cvr_sem)
    own_k = pltpu.make_async_copy(ck_of(t), ckr.at[t], c_sem.at[0])
    own_v = pltpu.make_async_copy(cv_of(t), cvr.at[t], c_sem.at[1])
    own_k.start()
    own_v.start()
    for c in loads[3:]:
        c.start()

    spread_wait(xg, xs_sem, xr_sem, xf_sem, xh_sem)

    def squares(c, acc):
        v = xg[c].astype(F32)
        return acc + jnp.sum(v * v, axis=1, keepdims=True)

    total = lax.fori_loop(0, peers, squares, jnp.zeros((seqs, 1), F32))
    factor = lax.rsqrt(total / model + epsilon)
    for c in loads[:3]:
        c.wait()

    def project(c, carry):
        q, k, v = carry
        at = pl.ds(pl.multiple_of(c * (4 * width), 4 * width), 4 * width)
        raw = jnp.concatenate([xg[c * 4 + i] for i in range(4)], axis=1).astype(F32)
        n = (raw * factor * gain1_ref[:, at]).astype(BF16)
        q = q + matmul(n, wq[at, :])
        k = k + lax.dot_general(n, wk[:, at], NT, preferred_element_type=F32)
        v = v + lax.dot_general(n, wv[:, at], NT, preferred_element_type=F32)
        return q, k, v

    kvw = wk.shape[0]
    q, k, v = lax.fori_loop(
        0,
        peers // 4,
        project,
        (
            jnp.zeros((seqs, width), F32),
            jnp.zeros((seqs, kvw), F32),
            jnp.zeros((seqs, kvw), F32),
        ),
    )
    parts = HD // kvw
    lane = lax.broadcasted_iota(jnp.int32, (seqs, HD), 1)
    mine = lane // kvw == lax.rem(t, parts)
    qkv[:, :width] = q.astype(BF16).astype(F32)
    for n, value in enumerate((k, v)):
        whole = jnp.concatenate([value.astype(BF16).astype(F32)] * parts, axis=1)
        qkv[:, width + n * HD : width + (n + 1) * HD] = jnp.where(mine, whole, 0.0)
    for d in range(tp_n):
        qs[d] = qkv[d * own : (d + 1) * own, :]
    qr[t] = qs[t]
    send_tp(lambda peer: qs.at[peer], qr, qs_sem, qr_sem)

    loads[3].wait()
    strip = 2 * HD

    def relay(n, carry):
        base = pl.multiple_of(n * strip, strip)
        flat = wo[pl.ds(base, strip)].reshape(strip, sub_n * width)
        for c in range(sub_n):
            wq[pl.ds(base + c * half, strip), :] = flat[:, c * width : (c + 1) * width]
        return carry

    lax.fori_loop(0, half // strip, relay, 0)

    wait_tp(ckr, cks_sem, ckr_sem)
    wait_tp(cvr, cvs_sem, cvr_sem)
    own_k.wait()
    own_v.wait()
    wait_tp(qr, qs_sem, qr_sem)

    rows = hpd * tp_n
    cols = tp_n * span * kvh
    row = lax.broadcasted_iota(jnp.int32, (rows, cols), 0)
    col = lax.broadcasted_iota(jnp.int32, (rows, cols), 1)
    same_head = lax.rem(row, tp_n) // parts == lax.rem(col, kvh)
    place = (col // kvh).astype(F32)
    pair_row = lax.broadcasted_iota(jnp.int32, (tp_n, tp_n), 0)
    pair_col = lax.broadcasted_iota(jnp.int32, (tp_n, tp_n), 1)
    pairs = jnp.where(pair_row // parts == pair_col // parts, 1.0, 0.0).astype(F32)
    root = math.sqrt(HD)

    def rope(value, cosine, sine):
        turned = pltpu.roll(value, HD // 2, 1)
        return (value * cosine + turned * sine).astype(BF16)

    for i in range(own):
        table = aux_ref[t * own + i]
        cosine, sine, length = table[0:1], table[1:2], table[2:3, 0:1]
        queries = jnp.concatenate(
            [qr[:, i, j * HD : (j + 1) * HD] for j in range(hpd)], axis=0
        )
        query_rot = rope(queries, cosine, sine)
        exact = lax.Precision.HIGHEST
        key_new = jnp.dot(
            pairs, qr[:, i, width : width + HD], precision=exact, preferred_element_type=F32
        )
        value_new = jnp.dot(
            pairs,
            qr[:, i, width + HD : width + 2 * HD],
            precision=exact,
            preferred_element_type=F32,
        )
        key_rot = rope(key_new, cosine, sine).astype(F32)
        keys = ckr[:, i].reshape(cols, HD)
        values = cvr[:, i].reshape(cols, HD).astype(F32)
        scores = lax.dot_general(query_rot, keys, NT, preferred_element_type=F32) / root
        live = same_head & (place < length)
        masked = jnp.where(live, scores, floor_score)
        key_all = jnp.concatenate([key_rot] * hpd, axis=0)
        value_all = jnp.concatenate([value_new] * hpd, axis=0)
        own_score = jnp.sum(query_rot.astype(F32) * key_all, axis=1, keepdims=True) / root
        highest = jnp.maximum(jnp.max(masked, axis=1, keepdims=True), own_score)
        weights = jnp.where(live, jnp.exp(masked - highest), 0.0)
        own_weight = jnp.exp(own_score - highest)
        numerator = jnp.dot(weights, values, precision=exact, preferred_element_type=F32)
        numerator = numerator + own_weight * value_all
        denominator = jnp.sum(weights, axis=1, keepdims=True) + own_weight
        ascr[...] = numerator / denominator
        for j in range(hpd):
            for d in range(tp_n):
                r = j * tp_n + d
                head = d * hpd + j
                arow[i : i + 1, head * HD : (head + 1) * HD] = ascr[r : r + 1, :]
    ab[t] = arow[...].astype(BF16)
    send_tp(lambda peer: ab.at[t], ab, as_sem, ar_sem)
    wait_tp(ab, as_sem, ar_sem)
    for d in range(tp_n):
        attf[d * own : (d + 1) * own, :] = ab[d].astype(F32)
    attb[...] = attf[...].astype(BF16)

    attended = attb[...]

    def mix(c, carry):
        op[c] = matmul(attended, wq[pl.ds(pl.multiple_of(c * half, half), half), :])
        return carry

    lax.fori_loop(0, sub_n, mix, 0)
    swap = remote(op.at[other], orv, o_sem.at[0], o_sem.at[1], t, other)
    swap.start()
    swap.wait_recv()
    middle = (x_ref[...].astype(F32) + (op[s] + orv[...])).astype(BF16)
    mg[me] = middle
    spread(mg.at[me], mg, ms_sem, mr_sem, mf_sem, mh_sem)
    spread_wait(mg, ms_sem, mr_sem, mf_sem, mh_sem)

    def squares_mid(c, acc):
        v = mg[c].astype(F32)
        return acc + jnp.sum(v * v, axis=1, keepdims=True)

    total_mid = lax.fori_loop(0, peers, squares_mid, jnp.zeros((seqs, 1), F32))
    factor_mid = lax.rsqrt(total_mid / model + epsilon)

    def scale(c, carry):
        at = pl.ds(pl.multiple_of(c * width, width), width)
        gain_at = pl.ds(pl.multiple_of(s * half + c * width, width), width)
        raw = mg[s * tp_n + c].astype(F32)
        nf[:, at] = (raw * factor_mid * gain2_ref[:, gain_at]).astype(BF16)
        return carry

    lax.fori_loop(0, tp_n, scale, 0)
    loads[4].wait()
    loads[5].wait()
    chunks, _, _, chunk = gp.shape

    def gate_copy(n):
        return remote(gp.at[n], gr.at[n], gs_sem.at[n], gr_sem.at[n], t, other)

    def gates(n, carry):
        at = pl.ds(pl.multiple_of(n * chunk, chunk), chunk)
        normed = nf[...]
        gp[n, 0] = matmul(normed, wg[:, at])
        gp[n, 1] = matmul(normed, wu[:, at])
        gate_copy(n).start()
        return carry

    lax.fori_loop(0, chunks, gates, 0)

    def joins(n, carry):
        gate_copy(n).wait_recv()
        at = pl.ds(pl.multiple_of(n * chunk, chunk), chunk)
        gate = gp[n, 0] + gr[n, 0]
        up = gp[n, 1] + gr[n, 1]
        hid[:, at] = (gate / (1.0 + jnp.exp(-gate)) * up).astype(BF16)
        return carry

    lax.fori_loop(0, chunks, joins, 0)
    loads[6].wait()

    def down(peer):
        at = pl.ds(pl.multiple_of(peer * width, width), width)
        return matmul(hid[...], wd[:, at])

    def share(k, carry):
        peer = lax.rem(t + k, tp_n)
        dp[peer] = down(peer).astype(BF16)
        remote(dp.at[peer], dr.at[t], ds_sem.at[k], dr_sem.at[t], peer, s).start()
        return carry

    lax.fori_loop(1, tp_n, share, 0)
    result = down(t)

    def gather(k, acc):
        peer = lax.rem(t + k, tp_n)
        remote(dr.at[peer], dr.at[peer], ds_sem.at[k], dr_sem.at[peer], t, s).wait_recv()
        return acc + dr[peer].astype(F32)

    result = lax.fori_loop(1, tp_n, gather, result)
    out_ref[...] = (mg[me].astype(F32) + result).astype(BF16)

    spread_done(x_ref, xg, xs_sem, xr_sem, xf_sem, xh_sem)
    done_tp(ck_of, ckr, cks_sem, ckr_sem)
    done_tp(cv_of, cvr, cvs_sem, cvr_sem)
    done_tp(lambda peer: qs.at[peer], qr, qs_sem, qr_sem)
    done_tp(lambda peer: ab.at[t], ab, as_sem, ar_sem)
    swap.wait_send()
    spread_done(mg.at[me], mg, ms_sem, mr_sem, mf_sem, mh_sem)

    def gates_done(n, carry):
        gate_copy(n).wait_send()
        return carry

    lax.fori_loop(0, chunks, gates_done, 0)
    done_tp(lambda peer: dp.at[peer], dr, ds_sem, dr_sem)


def per_device(
    hidden_in,
    norm_attn,
    w_query,
    w_key,
    w_value,
    w_out,
    norm_ffn,
    w_gate,
    w_up,
    w_down,
    cache_keys,
    cache_values,
    lengths,
):
    tp_n = lax.axis_size("tp")
    sub_n = lax.axis_size("sub")
    seqs, _, width = hidden_in.shape
    model = norm_attn.shape[0]
    half = width * tp_n
    kvw = w_key.shape[2]
    span, kvh = cache_keys.shape[1:3]
    ff = w_gate.shape[2]
    hpd = max(width // HD, 1)
    own = max(seqs // tp_n, 1)
    fits = (
        sub_n == 2
        and tp_n % 2 == 0
        and width % HD == 0
        and ff % HD == 0
        and seqs % tp_n == 0
        and HD % kvw == 0
        and w_query.shape[2] == width
        and hpd * (HD // kvw) * kvh == hpd * tp_n
        and (span * kvh) % 16 == 0
    )
    if not fits:
        return per_device_plain(
            hidden_in,
            norm_attn,
            w_query,
            w_key,
            w_value,
            w_out,
            norm_ffn,
            w_gate,
            w_up,
            w_down,
            cache_keys,
            cache_values,
            lengths,
        )
    peers = tp_n * sub_n
    angles = rope_angles(lengths)
    cosine = jnp.cos(angles)
    sine = jnp.sin(angles)
    long = jnp.broadcast_to(lengths.astype(F32)[:, None], (seqs, HD))
    aux = jnp.stack(
        [
            jnp.concatenate([cosine, cosine], axis=1),
            jnp.concatenate([-sine, sine], axis=1),
            long,
        ],
        axis=1,
    )
    aux = jnp.pad(aux, ((0, 0), (0, 5), (0, 0)))
    chunk = ff // 2 if ff % (2 * HD) == 0 else ff
    chunks = ff // chunk
    dma = pltpu.SemaphoreType.DMA
    vmem = pltpu.VMEM
    weights = [
        w_query.reshape(model, width),
        w_key.reshape(model, kvw).T,
        w_value.reshape(model, kvw).T,
        w_out.reshape(half, sub_n, width),
        w_gate.reshape(half, ff),
        w_up.reshape(half, ff),
        w_down.reshape(ff, half),
    ]
    caches = [
        cache_keys.reshape(seqs, span * kvh, HD),
        cache_values.reshape(seqs, span * kvh, HD),
    ]
    wide = width + 2 * HD
    out = pl.pallas_call(
        functools.partial(step_kernel, (tp_n, sub_n, own, hpd, span, kvh)),
        out_shape=jax.ShapeDtypeStruct((seqs, width), BF16),
        in_specs=[pl.BlockSpec(memory_space=pltpu.VMEM)] * 4
        + [pl.BlockSpec(memory_space=pl.ANY)] * 9,
        out_specs=pl.BlockSpec(memory_space=pltpu.VMEM),
        scratch_shapes=[vmem(w.shape, BF16) for w in weights]
        + [
            vmem((peers, seqs, width), BF16),
            vmem((tp_n, own, span * kvh, HD), BF16),
            vmem((tp_n, own, span * kvh, HD), BF16),
            vmem((seqs, wide), F32),
            vmem((tp_n, own, wide), F32),
            vmem((tp_n, own, wide), F32),
            vmem((hpd * tp_n, HD), F32),
            vmem((own, half), F32),
            vmem((tp_n, own, half), BF16),
            vmem((seqs, half), F32),
            vmem((seqs, half), BF16),
            vmem((sub_n, seqs, width), F32),
            vmem((seqs, width), F32),
            vmem((peers, seqs, width), BF16),
            vmem((seqs, half), BF16),
            vmem((chunks, 2, seqs, chunk), F32),
            vmem((chunks, 2, seqs, chunk), F32),
            vmem((seqs, ff), BF16),
            vmem((tp_n, seqs, width), BF16),
            vmem((tp_n, seqs, width), BF16),
            dma((7,)),
            dma((2,)),
            dma((tp_n,)),
            dma((tp_n,)),
            dma((tp_n,)),
            dma((tp_n,)),
            dma((tp_n,)),
            dma((tp_n,)),
            dma((tp_n,)),
            dma((tp_n,)),
            dma((tp_n,)),
            dma((tp_n,)),
            dma((2,)),
            dma((tp_n,)),
            dma((tp_n,)),
            dma((chunks,)),
            dma((chunks,)),
            dma((tp_n,)),
            dma((tp_n,)),
            dma((tp_n,)),
            dma((tp_n,)),
            dma((tp_n,)),
            dma((tp_n,)),
        ],
        compiler_params=pltpu.CompilerParams(
            collective_id=0, has_side_effects=True, vmem_limit_bytes=67043328
        ),
        name="decode_step",
    )(
        hidden_in.reshape(seqs, width),
        aux,
        norm_attn.reshape(1, model),
        norm_ffn.reshape(1, model),
        *weights,
        *caches,
    )
    return out.reshape(seqs, 1, width)


def solution(mesh):
    in_specs = (
        P("grp", "sub", "tp"),
        P(),
        P(None, "sub", "tp"),
        P(None, "sub", "tp"),
        P(None, "sub", "tp"),
        P("sub", None, None, "tp"),
        P(),
        P("sub", None, "tp"),
        P("sub", None, "tp"),
        P("tp", "sub", None),
        P("grp", "tp", "sub", None),
        P("grp", "tp", "sub", None),
        P("grp"),
    )
    out_specs = P("grp", "sub", "tp")
    return jax.shard_map(
        per_device, mesh=mesh, in_specs=in_specs, out_specs=out_specs, check_vma=False
    )
```
